256 devices in a mesh: grid: 64 (over z, x, core), band: 4 (over y).
Axes of the slice: x: 4, y: 4, z: 8, core: 2. Of those that a mesh axis runs over, the one named last changes fastest.
Arguments:
- basis: float32 [2048, 65536], P('band', 'grid'), as said below
- panel: float32 [1024, 65536], P('band', 'grid'), may hold values from -6 to 6
Outputs:
- new_panel: float32 [1024, 65536], P('band', 'grid')
- coeffs: float32 [2048, 1024], P('band')
The draws below stay inside these ranges and needn't reach their ends.
Inputs may be any that keep to these rules, and one draw needn't show every extreme that they name: The rows of basis are orthogonal to each other, each with squared sum 65536 (to float32 rounding).
All inputs are finite; a program needn't handle non-finite values.
Results may differ from the reference program's by a relative error of at most 0.000073.
Values sent between devices are 32-bit elements; how exact they have to be, the bound alone decides.
No kernel may reach another device: no remote copies, remote signals or barrier semaphores. Data moves between devices by JAX's collectives and lax.ppermute only.
A program may use at most 128 MiB of HBM per device.

```python
import jax
import jax.numpy as jnp
from jax import lax

NQ = 2048
NP = 1024
NG = 65536


def draw_basis(key, part):
    sample = jax.random.normal(key, (NG, NQ), jnp.float32)
    ortho, upper = jnp.linalg.qr(sample)
    return (ortho.T * jnp.sqrt(jnp.float32(NG))).astype(jnp.float32)


def shard_levels(key, dims, split, least, high):
    def one(axis_at, blocks):
        steps = jax.random.uniform(jax.random.fold_in(jax.random.fold_in(key, 6), axis_at), (blocks,), jnp.float32, least / len(split), high / len(split))
        return jnp.repeat(jnp.exp(steps), dims[axis_at] // blocks).reshape((-1,) + (1,) * (len(dims) - axis_at - 1))

    loudness = one(*split[0])
    for cut in split[1:]:
        loudness = loudness * one(*cut)
    return loudness


def noise(key, shape, width, bound, shards=(), kind=jnp.bfloat16):
    array = jax.random.normal(key, shape, jnp.float32) * width
    if len(shards) > 0:
        array = shard_levels(key, shape, shards, -0.22, 0.18) * array
    return jnp.clip(array, min=-bound, max=bound).astype(kind)


def setup_inputs(seed: int = 0) -> dict:
    key_list = jax.random.split(jax.random.key(seed), 3)
    basis = draw_basis(jax.random.fold_in(key_list[2], 71), 0)
    panel = noise(key_list[1], (NP, NG), 1.0, 6.0, ((0, 4), (1, 64)), jnp.float32)
    return dict(basis=basis, panel=panel)


def reference(basis, panel):
    highest = lax.Precision.HIGHEST
    n_grid = basis.shape[1]
    coeffs = jnp.dot(basis, panel.T, precision=highest) / n_grid
    projected = panel - jnp.dot(coeffs.T, basis, precision=highest)
    gram = jnp.dot(projected, projected.T, precision=highest) / n_grid
    factor = jnp.linalg.cholesky(gram)
    new_panel = lax.linalg.triangular_solve(factor, projected, left_side=True, lower=True)
    return (new_panel, coeffs)
```

```python
import jax
import jax.numpy as jnp
from jax import lax
from jax.experimental import pallas as pl
from jax.experimental.pallas import tpu as pltpu
from jax.sharding import Mesh, PartitionSpec as P

Z, X, C, B = 8, 4, 2, 4
GRID = ("z", "x", "c")
BLK = 128
HI = lax.Precision.HIGHEST
F32 = jnp.float32
VMEM = pl.BlockSpec(memory_space=pltpu.VMEM)
SMEM = pl.BlockSpec(memory_space=pltpu.SMEM)


def params(mib):
    return pltpu.CompilerParams(vmem_limit_bytes=mib * 1024 * 1024)


def shift(array, axis, count, by):
    return lax.ppermute(array, axis, [(i, (i + by) % count) for i in range(count)])


def tdot(left, right):
    return lax.dot_general(left, right, (((1,), (1,)), ((), ())), precision=HI, preferred_element_type=F32)


def cdot(left, right):
    return lax.dot_general(left, right, (((0,), (0,)), ((), ())), precision=HI, preferred_element_type=F32)


def rotate_body(ids_ref, basis_ref, panel_ref, out_ref):
    c, x, z = ids_ref[1], ids_ref[2], ids_ref[3]

    def place(t):
        return lax.rem(x + lax.rem(t // Z, X), X) * Z + lax.rem(z + lax.rem(t, Z), Z)

    def from_basis(t, carry):
        out_ref[t] = basis_ref[lax.rem(c + t // (X * Z), C) * (X * Z) + place(t)]
        return carry

    def from_panel(t, carry):
        out_ref[C * X * Z + t] = panel_ref[place(t)]
        return carry

    lax.fori_loop(0, C * X * Z, from_basis, 0)
    lax.fori_loop(0, X * Z, from_panel, 0)


def rotate(ids, basis, panel):
    nq, pts = basis.shape
    np_, _ = panel.shape
    out = pl.pallas_call(
        rotate_body,
        out_shape=jax.ShapeDtypeStruct(((nq + np_) // 8, 8, pts), F32),
        in_specs=[SMEM, VMEM, VMEM],
        out_specs=VMEM,
        compiler_params=params(16),
        name="rotate",
    )(ids, basis.reshape(nq // 8, 8, pts), panel.reshape(np_ // 8, 8, pts))
    return out.reshape(nq + np_, pts)


def unrotate_body(ids_ref, near_ref, far_ref, out_ref):
    b, c, x, z = ids_ref[0], ids_ref[1], ids_ref[2], ids_ref[3]
    width = out_ref.shape[2] // B
    for dc, ref in ((0, near_ref), (1, far_ref)):

        def one(t, carry):
            xx = lax.rem(x + t // Z, X)
            zz = lax.rem(z + lax.rem(t, Z), Z)
            dst = (lax.rem(c + dc, C) * X + xx) * Z + zz
            for s in range(B):
                at = pl.multiple_of(lax.rem(b + s, B) * width, width)
                out_ref[dst, :, pl.ds(at, width)] = ref[t, :, s * width : (s + 1) * width]
            return carry

        lax.fori_loop(0, X * Z, one, 0)


def unrotate(ids, near, far):
    rows, cols = near.shape
    out = pl.pallas_call(
        unrotate_body,
        out_shape=jax.ShapeDtypeStruct((2 * rows // 8, 8, cols), F32),
        in_specs=[SMEM, VMEM, VMEM],
        out_specs=VMEM,
        compiler_params=params(16),
        name="unrotate",
    )(ids, near.reshape(rows // 8, 8, cols), far.reshape(rows // 8, 8, cols))
    return out.reshape(2 * rows, cols)


def squares_body(ids_ref, near_ref, far_ref, out_ref, acc_ref):
    c, x, z = ids_ref[1], ids_ref[2], ids_ref[3]
    width = near_ref.shape[1] // B
    row = x * (8 * Z) + z * 8
    block = row // BLK
    inner = pl.multiple_of(row - block * BLK, 8)
    for s in range(B):
        at = pl.multiple_of(s * width + block * BLK, BLK)
        acc_ref[...] = cdot(near_ref[:, pl.ds(at, BLK)], near_ref[...]) + cdot(far_ref[:, pl.ds(at, BLK)], far_ref[...])
        for h in range(2):
            a = (s + h) % B
            d = (s + 2 + h) % B
            low = acc_ref[pl.ds(inner, 8), a * width : (a + 1) * width]
            high = acc_ref[pl.ds(inner, 8), d * width : (d + 1) * width]
            out_ref[s, :, h * width : (h + 1) * width] = jnp.where(c == 0, low, high)


def squares(ids, near, far):
    cols = near.shape[1]
    return pl.pallas_call(
        squares_body,
        out_shape=jax.ShapeDtypeStruct((B, 8, cols // 2), F32),
        in_specs=[SMEM, VMEM, VMEM],
        out_specs=VMEM,
        scratch_shapes=[pltpu.VMEM((BLK, cols), F32)],
        compiler_params=params(24),
        name="squares",
    )(ids, near, far)


def project_body(ids_ref, near_ref, far_ref, basis_ref, panel_ref, out_ref):
    half = near_ref.shape[0]
    out_ref[...] = cdot(near_ref[...], basis_ref[:half]) + cdot(far_ref[...], basis_ref[half:])

    @pl.when(pl.program_id(0) == 0)
    def _():
        out_ref[...] = out_ref[...] - panel_ref[...]


def project(ids, near, far, stacked, panel):
    half, cols = near.shape
    rows, pts = panel.shape
    return pl.pallas_call(
        project_body,
        out_shape=jax.ShapeDtypeStruct((cols, pts), F32),
        grid_spec=pltpu.PrefetchScalarGridSpec(
            num_scalar_prefetch=1,
            grid=(B,),
            in_specs=[
                pl.BlockSpec((half, rows), lambda s, ids: (0, s)),
                pl.BlockSpec((half, rows), lambda s, ids: (0, s)),
                pl.BlockSpec((2 * half, pts), lambda s, ids: (0, 0)),
                pl.BlockSpec((rows, pts), lambda s, ids: (0, 0)),
            ],
            out_specs=pl.BlockSpec((rows, pts), lambda s, ids: (lax.rem(ids[0] + s, B), 0)),
        ),
        compiler_params=params(32),
        name="project",
    )(ids, near, far, stacked, panel)


def lane_splat(tile, c):
    return jnp.broadcast_to(tile[:, c : c + 1], tile.shape)


def row_splat(tile, k):
    return jnp.broadcast_to(tile[k : k + 1, :], tile.shape)


def unit_inverse(tiles):
    n = len(tiles)
    tiles = list(tiles)
    sub = lax.broadcasted_iota(jnp.int32, (8, BLK), 0)
    lane = lax.broadcasted_iota(jnp.int32, (8, BLK), 1)
    zero = jnp.zeros((8, BLK), F32)
    one = jnp.ones((8, BLK), F32)
    scale = [None] * n
    for jb in range(n):
        j0 = 8 * jb
        inside = (lane >= j0) & (lane < j0 + 8)
        cols = {r: [lane_splat(tiles[r], j0 + k) for k in range(8)] for r in range(jb, n)}
        panel = jnp.where(inside, jnp.where(lane - j0 == sub, one, zero), tiles[jb])
        mult = {r: [None] * 8 for r in range(jb, n)}
        rows = []
        diag = zero
        for k in range(8):
            pivot = row_splat(cols[jb][k], k)
            recip = 1.0 / pivot
            diag = jnp.where(sub == k, pivot, diag)
            row = row_splat(panel, k)
            rows.append(row)
            for r in range(jb, n):
                m = cols[r][k] * recip
                mult[r][k] = jnp.where(sub > k, m, zero) if r == jb else m
            if k < 7:
                panel = panel - mult[jb][k] * row
            for q in range(k + 1, 8):
                f = row_splat(cols[jb][q], k)
                for r in range(jb, n):
                    cols[r][q] = cols[r][q] - mult[r][k] * f
        for r in range(jb + 1, n):
            a = jnp.where(inside, zero, tiles[r])
            for k in range(8):
                a = a - mult[r][k] * rows[k]
            tiles[r] = a
        tiles[jb] = panel
        scale[jb] = lax.rsqrt(diag)
    return [jnp.where(lane <= 8 * r + sub, tiles[r], zero) * scale[r] for r in range(n)]


def factor_body(ids_ref, near_ref, far_ref, out_ref, m_ref, r_ref):
    b, c, x, z = ids_ref[0], ids_ref[1], ids_ref[2], ids_ref[3]
    nb = m_ref.shape[0]
    per_band = nb // B
    for dc, ref in ((0, near_ref), (1, far_ref)):
        cc = lax.rem(c + dc, C)

        def take(t, carry):
            xx = lax.rem(x + t // Z, X)
            zz = lax.rem(z + lax.rem(t, Z), Z)
            for db in range(B):
                bb = lax.rem(b + db, B)
                row = pl.multiple_of(bb * (per_band * BLK) + (xx * Z + zz) * 8, 8)
                for m in range(nb // 2):
                    col = lax.rem(bb + 2 * cc + m // per_band, B) * per_band + m % per_band
                    m_ref[col, pl.ds(row, 8), :] = ref[t * B + db, :, m * BLK : (m + 1) * BLK]
            return carry

        lax.fori_loop(0, X * Z, take, 0)

    def step(k, carry):
        base = pl.multiple_of(k * BLK, BLK)
        tiles = [m_ref[k, pl.ds(base + 8 * r, 8), :] for r in range(BLK // 8)]
        inv = jnp.concatenate(unit_inverse(tiles), 0)
        line = jnp.concatenate([m_ref[cb, pl.ds(base, BLK), :] for cb in range(nb)], 1)
        prod = jnp.dot(inv, line, precision=HI, preferred_element_type=F32)
        for cb in range(nb):
            r_ref[cb] = jnp.where(cb == k, inv, prod[:, cb * BLK : (cb + 1) * BLK])

        @pl.when(k // per_band == b)
        def _():
            at = pl.multiple_of(lax.rem(k, per_band) * BLK, BLK)
            for cb in range(nb):
                out_ref[pl.ds(at, BLK), cb * BLK : (cb + 1) * BLK] = jnp.where(cb <= k, -r_ref[cb], 0.0)

        m_ref[k] = jnp.zeros(m_ref.shape[1:], F32)

        def trail(i, carry):
            ib = pl.multiple_of(i * BLK, BLK)
            full = jnp.concatenate([r_ref[cb] for cb in range(nb)], 1)
            update = cdot(r_ref[i], full)
            for cb in range(nb):
                m_ref[cb, pl.ds(ib, BLK), :] = m_ref[cb, pl.ds(ib, BLK), :] - update[:, cb * BLK : (cb + 1) * BLK]
            return carry

        lax.fori_loop(k + 1, nb, trail, 0)
        return carry

    lax.fori_loop(0, nb, step, 0)


def factor_rows(ids, near, far, n):
    return pl.pallas_call(
        factor_body,
        out_shape=jax.ShapeDtypeStruct((n // B, n), F32),
        in_specs=[SMEM, VMEM, VMEM],
        out_specs=VMEM,
        scratch_shapes=[pltpu.VMEM((n // BLK, n, BLK), F32), pltpu.VMEM((n // BLK, BLK, BLK), F32)],
        compiler_params=params(40),
        name="factor_rows",
    )(ids, near, far)


def spread(count):
    return [(s, s if 2 * s <= count else s - count) for s in range(1, count)]


def ring4(piece, axis):
    half = piece.shape[0] // 2
    after = shift(piece, axis, 4, -1)
    before = shift(piece, axis, 4, 1)
    low = shift(after[:half], axis, 4, -1)
    high = shift(before[half:], axis, 4, 1)
    return [piece, after, jnp.concatenate([low, high], 0), before]


def gather_z(piece):
    return [piece] + [shift(piece, "z", Z, -by) for _, by in spread(Z)]


def body(basis, panel):
    rows_p, pts = panel.shape
    n_panel = rows_p * B
    n_grid = pts * Z * X * C
    core = lax.axis_index("c")
    ids = jnp.stack([lax.axis_index(a) for a in ("b", "c", "x", "z")]).astype(jnp.int32)
    chunks = ring4(panel, "b")
    stacked = rotate(ids, basis, panel)
    rows_q = basis.shape[0]
    half_q = rows_q // 2
    parts = [tdot(stacked, chunk) for chunk in chunks]
    grams = [part[rows_q:] for part in parts]
    first = core == 0
    keep = [part[:half_q] for part in parts] + [jnp.where(first, grams[i], grams[i + 2]) for i in range(2)]
    give = [part[half_q:rows_q] for part in parts] + [jnp.where(first, grams[i + 2], grams[i]) for i in range(2)]
    mine = jnp.concatenate(keep, 1) + shift(jnp.concatenate(give, 1), "c", C, 1)
    wide = mine.shape[1]
    mine = mine.reshape(X, -1, wide)
    mid = mine.shape[1] // 2
    far2 = jnp.concatenate([shift(mine[2, :mid], "x", X, 2), shift(mine[2, mid:], "x", X, -2)], 0)
    mine = mine[0] + shift(mine[1], "x", X, 1) + shift(mine[3], "x", X, -1) + far2
    mine = mine.reshape(Z, -1, wide)
    total = mine[0]
    for s, by in spread(Z):
        total = total + shift(mine[s], "z", Z, by)
    total = total / n_grid
    own = total[:, :n_panel]
    own_gram = total[:, n_panel:]

    own = jnp.concatenate(gather_z(own), 0)
    near = jnp.concatenate(ring4(own, "x"), 0)
    far = shift(near, "c", C, 1)

    pieces = squares(ids, near, far)
    own_gram = own_gram - pieces[0]
    for s, by in spread(B):
        own_gram = own_gram - shift(pieces[s], "b", B, by)
    own_gram = jnp.concatenate([own_gram] + [shift(own_gram, "b", B, -by) for _, by in spread(B)], 0)
    own_gram = jnp.concatenate(gather_z(own_gram), 0)
    near_gram = jnp.concatenate(ring4(own_gram, "x"), 0)
    far_gram = shift(near_gram, "c", C, 1)

    short = lax.psum(project(ids, near, far, stacked[:rows_q], panel), "b")
    coeffs = unrotate(ids, near, far)
    tiled = (-1, 8, near_gram.shape[1])
    rows = factor_rows(ids, near_gram.reshape(tiled), far_gram.reshape(tiled), n_panel)
    new_panel = jnp.dot(rows, short, precision=HI, preferred_element_type=F32)
    return (new_panel, coeffs)


def solution(mesh):
    fine = Mesh(mesh.devices.reshape(Z, X, C, B), GRID + ("b",))
    placed = (P("b", GRID), P("b", GRID))
    return jax.shard_map(
        body,
        mesh=fine,
        in_specs=placed,
        out_specs=(P("b", GRID), P("b", None)),
        check_vma=False,
    )
```

```python
import jax
import jax.numpy as jnp
from jax import lax
from jax.experimental import pallas as pl
from jax.experimental.pallas import tpu as pltpu
from jax.sharding import Mesh, PartitionSpec as P


Z, X, C, B = 8, 4, 2, 4
GRID = ("z", "x", "c")
BLK = 128
HI = lax.Precision.HIGHEST
F32 = jnp.float32
VMEM = pl.BlockSpec(memory_space=pltpu.VMEM)
SMEM = pl.BlockSpec(memory_space=pltpu.SMEM)


def params(mib):
    return pltpu.CompilerParams(vmem_limit_bytes=mib * 1024 * 1024)


def shift(array, axis, count, by):
    return lax.ppermute(array, axis, [(i, (i + by) % count) for i in range(count)])


def z_at(z, p):
    e = p // 2
    return lax.rem(z + e + 4 * lax.rem(p, 2) + 4 * (e // 3), Z)


def tdot(left, right):
    return lax.dot_general(left, right, (((1,), (1,)), ((), ())), precision=HI, preferred_element_type=F32)


def cdot(left, right):
    return lax.dot_general(left, right, (((0,), (0,)), ((), ())), precision=HI, preferred_element_type=F32)


def rotate_body(ids_ref, basis_ref, panel_ref, out_ref):
    c, x, z = ids_ref[1], ids_ref[2], ids_ref[3]

    def place(t):
        return lax.rem(x + lax.rem(t // Z, X), X) * Z + z_at(z, lax.rem(t, Z))

    def from_basis(t, carry):
        out_ref[t] = basis_ref[lax.rem(c + t // (X * Z), C) * (X * Z) + place(t)]
        return carry

    def from_panel(t, carry):
        out_ref[C * X * Z + t] = panel_ref[place(t)]
        return carry

    lax.fori_loop(0, C * X * Z, from_basis, 0)
    lax.fori_loop(0, X * Z, from_panel, 0)


def rotate(ids, basis, panel):
    nq, pts = basis.shape
    np_, _ = panel.shape
    out = pl.pallas_call(
        rotate_body,
        out_shape=jax.ShapeDtypeStruct(((nq + np_) // 8, 8, pts), F32),
        in_specs=[SMEM, VMEM, VMEM],
        out_specs=VMEM,
        compiler_params=params(16),
        name="rotate",
    )(ids, basis.reshape(nq // 8, 8, pts), panel.reshape(np_ // 8, 8, pts))
    return out.reshape(nq + np_, pts)


def unrotate_body(ids_ref, near_ref, far_ref, out_ref):
    b, c, x, z = ids_ref[0], ids_ref[1], ids_ref[2], ids_ref[3]
    width = out_ref.shape[2] // B
    for dc, ref in ((0, near_ref), (1, far_ref)):

        def one(t, carry):
            xx = lax.rem(x + t // Z, X)
            zz = z_at(z, lax.rem(t, Z))
            dst = (lax.rem(c + dc, C) * X + xx) * Z + zz
            for s in range(B):
                at = pl.multiple_of(lax.rem(b + s, B) * width, width)
                out_ref[dst, :, pl.ds(at, width)] = ref[t, :, s * width : (s + 1) * width]
            return carry

        lax.fori_loop(0, X * Z, one, 0)


def unrotate(ids, near, far):
    rows, cols = near.shape
    out = pl.pallas_call(
        unrotate_body,
        out_shape=jax.ShapeDtypeStruct((2 * rows // 8, 8, cols), F32),
        in_specs=[SMEM, VMEM, VMEM],
        out_specs=VMEM,
        compiler_params=params(16),
        name="unrotate",
    )(ids, near.reshape(rows // 8, 8, cols), far.reshape(rows // 8, 8, cols))
    return out.reshape(2 * rows, cols)


def squares_body(ids_ref, near_ref, far_ref, gram_ref, out_ref, acc_ref):
    c, x, z = ids_ref[1], ids_ref[2], ids_ref[3]
    width = near_ref.shape[1] // B
    row = x * (8 * Z) + z * 8
    block = row // BLK
    inner = pl.multiple_of(row - block * BLK, 8)

    def one(s, carry):
        at = pl.multiple_of(s * width + block * BLK, BLK)
        acc_ref[...] = cdot(near_ref[:, pl.ds(at, BLK)], near_ref[...]) + cdot(far_ref[:, pl.ds(at, BLK)], far_ref[...])
        for m in range(B):
            col = pl.multiple_of(lax.rem(s + m, B) * width + c * BLK, BLK)
            base = jnp.where(s == 0, gram_ref[:, m * BLK : (m + 1) * BLK], 0.0)
            out_ref[s, :, m * BLK : (m + 1) * BLK] = base - acc_ref[pl.ds(inner, 8), pl.ds(col, BLK)]
        return carry

    lax.fori_loop(0, B, one, 0)


def squares(ids, near, far, gram):
    cols = near.shape[1]
    return pl.pallas_call(
        squares_body,
        out_shape=jax.ShapeDtypeStruct((B, 8, cols // 2), F32),
        in_specs=[SMEM, VMEM, VMEM, VMEM],
        out_specs=VMEM,
        scratch_shapes=[pltpu.VMEM((BLK, cols), F32)],
        compiler_params=params(24),
        name="squares",
    )(ids, near, far, gram)


def project_body(ids_ref, near_ref, far_ref, basis_ref, panel_ref, out_ref):
    half = near_ref.shape[0]
    out_ref[...] = cdot(near_ref[...], basis_ref[:half]) + cdot(far_ref[...], basis_ref[half:])

    @pl.when(pl.program_id(0) == 0)
    def _():
        out_ref[...] = out_ref[...] - panel_ref[...]


def project(ids, near, far, stacked, panel):
    half, cols = near.shape
    rows, pts = panel.shape
    return pl.pallas_call(
        project_body,
        out_shape=jax.ShapeDtypeStruct((cols, pts), F32),
        grid_spec=pltpu.PrefetchScalarGridSpec(
            num_scalar_prefetch=1,
            grid=(B,),
            in_specs=[
                pl.BlockSpec((half, rows), lambda s, ids: (0, s)),
                pl.BlockSpec((half, rows), lambda s, ids: (0, s)),
                pl.BlockSpec((2 * half, pts), lambda s, ids: (0, 0)),
                pl.BlockSpec((rows, pts), lambda s, ids: (0, 0)),
            ],
            out_specs=pl.BlockSpec((rows, pts), lambda s, ids: (lax.rem(ids[0] + s, B), 0)),
        ),
        compiler_params=params(32),
        name="project",
    )(ids, near, far, stacked, panel)


def lane_splat(tile, c):
    lane = lax.broadcasted_iota(jnp.int32, tile.shape, 1)
    return jnp.broadcast_to(jnp.sum(jnp.where(lane == c, tile, 0.0), axis=1, keepdims=True), tile.shape)


def row_splat(tile, k):
    return jnp.broadcast_to(tile[k : k + 1, :], tile.shape)


def unit_inverse(tiles):
    n = len(tiles)
    tiles = list(tiles)
    sub = lax.broadcasted_iota(jnp.int32, (8, BLK), 0)
    lane = lax.broadcasted_iota(jnp.int32, (8, BLK), 1)
    zero = jnp.zeros((8, BLK), F32)
    one = jnp.ones((8, BLK), F32)
    scale = [None] * n
    for jb in range(n):
        j0 = 8 * jb
        inside = (lane >= j0) & (lane < j0 + 8)
        cols = {r: [lane_splat(tiles[r], j0 + k) for k in range(8)] for r in range(jb, n)}
        panel = jnp.where(inside, jnp.where(lane - j0 == sub, one, zero), tiles[jb])
        mult = {r: [None] * 8 for r in range(jb, n)}
        rows = []
        diag = zero
        for k in range(8):
            pivot = row_splat(cols[jb][k], k)
            recip = 1.0 / pivot
            diag = jnp.where(sub == k, pivot, diag)
            row = row_splat(panel, k)
            rows.append(row)
            for r in range(jb, n):
                m = cols[r][k] * recip
                mult[r][k] = jnp.where(sub > k, m, zero) if r == jb else m
            if k < 7:
                panel = panel - mult[jb][k] * row
            for q in range(k + 1, 8):
                f = row_splat(cols[jb][q], k)
                for r in range(jb, n):
                    cols[r][q] = cols[r][q] - mult[r][k] * f
        for r in range(jb + 1, n):
            a = jnp.where(inside, zero, tiles[r])
            for k in range(8):
                a = a - mult[r][k] * rows[k]
            tiles[r] = a
        tiles[jb] = panel
        scale[jb] = lax.rsqrt(diag)
    return [jnp.where(lane <= 8 * r + sub, tiles[r], zero) * scale[r] for r in range(n)]


def three(x):
    high = x.astype(jnp.bfloat16)
    rest = x - high.astype(F32)
    mid = rest.astype(jnp.bfloat16)
    return high, mid, (rest - mid.astype(F32)).astype(jnp.bfloat16)


def six(left, right, axis):
    (h, m, l), (p, q, r) = left, right
    return jnp.concatenate([h, h, m, h, l, m], axis), jnp.concatenate([p, q, p, r, p, q], 0)


def factor_body(ids_ref, near_ref, far_ref, out_ref, m_ref, s_ref):
    b, c, x, z = ids_ref[0], ids_ref[1], ids_ref[2], ids_ref[3]
    nb = m_ref.shape[0]
    per_band = nb // B
    wide = 2
    for dc, ref in ((0, near_ref), (1, far_ref)):
        cc = lax.rem(c + dc, C)

        def take(t, carry):
            xx = lax.rem(x + t // Z, X)
            zz = z_at(z, lax.rem(t, Z))
            for db in range(B):
                bb = lax.rem(b + db, B)
                row = pl.multiple_of(bb * (per_band * BLK) + (xx * Z + zz) * 8, 8)
                for m in range(nb // 2):
                    col = lax.rem(bb + m, B) * per_band + cc
                    m_ref[col, pl.ds(row, 8), :] = ref[t * B + db, :, m * BLK : (m + 1) * BLK]
            return carry

        lax.fori_loop(0, X * Z, take, 0)

    def step(k, carry):
        base = pl.multiple_of(k * BLK, BLK)
        tiles = [m_ref[k, pl.ds(base + 8 * r, 8), :] for r in range(BLK // 8)]
        inv = jnp.concatenate(unit_inverse(tiles), 0)
        line = jnp.concatenate([m_ref[cb, pl.ds(base, BLK), :] for cb in range(nb)], 1)
        left, right = six(three(inv), three(line), 1)
        prod = jnp.dot(left, right, preferred_element_type=F32)
        blocks = [jnp.where(cb == k, inv, prod[:, cb * BLK : (cb + 1) * BLK]) for cb in range(nb)]

        @pl.when(k // per_band == b)
        def _():
            at = pl.multiple_of(lax.rem(k, per_band) * BLK, BLK)
            for cb in range(nb):
                out_ref[pl.ds(at, BLK), cb * BLK : (cb + 1) * BLK] = jnp.where(cb <= k, -blocks[cb], 0.0)

        for cb in range(nb):
            for i, term in enumerate(three(blocks[cb])):
                s_ref[cb, i * BLK : (i + 1) * BLK] = term
        m_ref[k] = jnp.zeros(m_ref.shape[1:], F32)

        def terms(x):
            return x[:BLK], x[BLK : 2 * BLK], x[2 * BLK :]

        def trail(i, carry):
            ib = pl.multiple_of(i * wide * BLK, wide * BLK)
            full = jnp.concatenate([s_ref[cb] for cb in range(nb)], 1)
            some = jnp.concatenate([s_ref[i * wide + w] for w in range(wide)], 1)
            left, right = six(terms(some), terms(full), 0)
            update = lax.dot_general(left, right, (((0,), (0,)), ((), ())), preferred_element_type=F32)
            for cb in range(nb):
                m_ref[cb, pl.ds(ib, wide * BLK), :] = (
                    m_ref[cb, pl.ds(ib, wide * BLK), :] - update[:, cb * BLK : (cb + 1) * BLK]
                )
            return carry

        lax.fori_loop((k + 1) // wide, jnp.where(k == nb - 1, 0, nb // wide), trail, 0)
        return carry

    lax.fori_loop(0, nb, step, 0)


def factor_rows(ids, near, far, n):
    return pl.pallas_call(
        factor_body,
        out_shape=jax.ShapeDtypeStruct((n // B, n), F32),
        in_specs=[SMEM, VMEM, VMEM],
        out_specs=VMEM,
        scratch_shapes=[pltpu.VMEM((n // BLK, n, BLK), F32), pltpu.VMEM((n // BLK, 3 * BLK, BLK), jnp.bfloat16)],
        compiler_params=params(40),
        name="factor_rows",
    )(ids, near, far)


def ring4(piece, axis):
    half = piece.shape[0] // 2
    after = shift(piece, axis, 4, -1)
    before = shift(piece, axis, 4, 1)
    low = shift(after[:half], axis, 4, -1)
    high = shift(before[half:], axis, 4, 1)
    return [piece, after, jnp.concatenate([low, high], 0), before]


def gather_z(piece):
    pair = jnp.concatenate([piece, shift(piece, "z", Z, 4)], 0)
    return jnp.concatenate([pair] + [shift(pair, "z", Z, by) for by in (-1, -2, 1)], 0)


def reduce_z(rows):
    pairs = rows.reshape(4, -1, rows.shape[1])
    total = pairs[0]
    for e, by in ((1, 1), (2, 2), (3, -1)):
        total = total + shift(pairs[e], "z", Z, by)
    half = total.shape[0] // 2
    return total[:half] + shift(total[half:], "z", Z, 4)


def reduce_core_x(parts, rows_q, first):
    half = rows_q // 2
    low = [part[rows_q:, :BLK] for part in parts]
    high = [part[rows_q:, BLK:] for part in parts]
    keep = [part[:half] for part in parts] + [jnp.where(first, a, d) for a, d in zip(low, high)]
    give = [part[half:rows_q] for part in parts] + [jnp.where(first, d, a) for a, d in zip(low, high)]
    mine = jnp.concatenate(keep, 1) + shift(jnp.concatenate(give, 1), "c", C, 1)
    mine = mine.reshape(X, -1, mine.shape[1])
    mid = mine.shape[1] // 2
    across = jnp.concatenate([shift(mine[2, :mid], "x", X, 2), shift(mine[2, mid:], "x", X, -2)], 0)
    return mine[0] + shift(mine[1], "x", X, 1) + shift(mine[3], "x", X, -1) + across


def body(basis, panel):
    rows_p, pts = panel.shape
    rows_q = basis.shape[0]
    n_panel = rows_p * B
    n_grid = pts * Z * X * C
    first = lax.axis_index("c") == 0
    ids = jnp.stack([lax.axis_index(a) for a in ("b", "c", "x", "z")]).astype(jnp.int32)
    chunks = ring4(panel, "b")
    stacked = rotate(ids, basis, panel)
    groups = ((0,), (1, 3), (2,))
    reduced = []
    for group in groups:
        parts = [tdot(stacked, chunks[s]) for s in group]
        reduced.append(reduce_core_x(parts, rows_q, first))
    total = reduce_z(jnp.concatenate(reduced, 1)) / n_grid
    coeff_at, gram_at, at = ({}, {}, 0)
    for group in groups:
        for s in group:
            coeff_at[s], at = (at, at + rows_p)
        for s in group:
            gram_at[s], at = (at, at + BLK)
    own = jnp.concatenate([total[:, coeff_at[s] : coeff_at[s] + rows_p] for s in range(B)], 1)
    own_gram = jnp.concatenate([total[:, gram_at[s] : gram_at[s] + BLK] for s in range(B)], 1)

    own = gather_z(own)
    near = jnp.concatenate(ring4(own, "x"), 0)
    far = shift(near, "c", C, 1)

    piece = squares(ids, near, far, own_gram)
    gram = piece
    for d in range(1, B):
        gram = gram + jnp.roll(shift(piece, "b", B, -d), d, 0)
    gram, short = lax.optimization_barrier((gram, project(ids, near, far, stacked[:rows_q], panel)))
    short = lax.psum(short, "b")
    gram = gather_z(gram.reshape(B * 8, -1))
    near_gram = jnp.concatenate(ring4(gram, "x"), 0)
    far_gram = shift(near_gram, "c", C, 1)

    coeffs = unrotate(ids, near, far)
    tiled = (-1, 8, near_gram.shape[1])
    rows = factor_rows(ids, near_gram.reshape(tiled), far_gram.reshape(tiled), n_panel)
    new_panel = jnp.dot(rows, short, precision=lax.Precision.HIGH, preferred_element_type=F32)
    return (new_panel, coeffs)


def solution(mesh):
    fine = Mesh(mesh.devices.reshape(Z, X, C, B), GRID + ("b",))
    placed = (P("b", GRID), P("b", GRID))
    return jax.shard_map(
        body,
        mesh=fine,
        in_specs=placed,
        out_specs=(P("b", GRID), P("b", None)),
        check_vma=False,
    )
```

```python
import jax
import jax.numpy as jnp
from jax import lax
from jax.experimental import pallas as pl
from jax.experimental.pallas import tpu as pltpu
from jax.sharding import Mesh, PartitionSpec as P


Z, X, C, B = 8, 4, 2, 4
GRID = ("z", "x", "c")
BLK = 128
HI = lax.Precision.HIGHEST
F32 = jnp.float32
VMEM = pl.BlockSpec(memory_space=pltpu.VMEM)
SMEM = pl.BlockSpec(memory_space=pltpu.SMEM)


def params(mib):
    return pltpu.CompilerParams(vmem_limit_bytes=mib * 1024 * 1024)


def shift(array, axis, count, by):
    return lax.ppermute(array, axis, [(i, (i + by) % count) for i in range(count)])


def two(x):
    high = x.astype(jnp.bfloat16)
    return high, (x - high.astype(F32)).astype(jnp.bfloat16)


def z_at(z, p):
    e = p // 2
    return lax.rem(z + e + 4 * lax.rem(p, 2) + 4 * (e // 3), Z)


def tdot(left, right):
    return lax.dot_general(left, right, (((1,), (1,)), ((), ())), precision=HI, preferred_element_type=F32)


def cdot(left, right):
    return lax.dot_general(left, right, (((0,), (0,)), ((), ())), precision=HI, preferred_element_type=F32)


def rotate_body(ids_ref, basis_ref, panel_ref, out_ref):
    c, x, z = ids_ref[1], ids_ref[2], ids_ref[3]

    def place(t):
        return lax.rem(x + lax.rem(t // Z, X), X) * Z + z_at(z, lax.rem(t, Z))

    def from_basis(t, carry):
        out_ref[t] = basis_ref[lax.rem(c + t // (X * Z), C) * (X * Z) + place(t)]
        return carry

    def from_panel(t, carry):
        out_ref[C * X * Z + t] = panel_ref[place(t)]
        return carry

    lax.fori_loop(0, C * X * Z, from_basis, 0)
    lax.fori_loop(0, X * Z, from_panel, 0)


def rotate(ids, basis, panel):
    nq, pts = basis.shape
    np_, _ = panel.shape
    out = pl.pallas_call(
        rotate_body,
        out_shape=jax.ShapeDtypeStruct(((nq + np_) // 8, 8, pts), F32),
        in_specs=[SMEM, VMEM, VMEM],
        out_specs=VMEM,
        compiler_params=params(16),
        name="rotate",
    )(ids, basis.reshape(nq // 8, 8, pts), panel.reshape(np_ // 8, 8, pts))
    return out.reshape(nq + np_, pts)


def unrotate_body(ids_ref, near_ref, far_ref, out_ref):
    b, c, x, z = ids_ref[0], ids_ref[1], ids_ref[2], ids_ref[3]
    width = out_ref.shape[2] // B
    for dc, ref in ((0, near_ref), (1, far_ref)):

        def one(t, carry):
            xx = lax.rem(x + t // Z, X)
            zz = z_at(z, lax.rem(t, Z))
            dst = (lax.rem(c + dc, C) * X + xx) * Z + zz
            for s in range(B):
                at = pl.multiple_of(lax.rem(b + s, B) * width, width)
                out_ref[dst, :, pl.ds(at, width)] = ref[t, :, s * width : (s + 1) * width]
            return carry

        lax.fori_loop(0, X * Z, one, 0)


def unrotate(ids, near, far):
    rows, cols = near.shape
    out = pl.pallas_call(
        unrotate_body,
        out_shape=jax.ShapeDtypeStruct((2 * rows // 8, 8, cols), F32),
        in_specs=[SMEM, VMEM, VMEM],
        out_specs=VMEM,
        compiler_params=params(16),
        name="unrotate",
    )(ids, near.reshape(rows // 8, 8, cols), far.reshape(rows // 8, 8, cols))
    return out.reshape(2 * rows, cols)


def squares_body(ids_ref, near_ref, far_ref, gram_ref, out_ref, acc_ref):
    c, x, z = ids_ref[1], ids_ref[2], ids_ref[3]
    width = near_ref.shape[1] // B
    row = x * (8 * Z) + z * 8
    block = row // BLK
    inner = row - block * BLK
    lane = lax.broadcasted_iota(jnp.int32, (near_ref.shape[0], BLK), 1)

    def rows_of(ref):
        rows = jnp.zeros((ref.shape[0], BLK), F32)
        for s in range(B):
            at = pl.multiple_of(s * width + block * BLK, BLK)
            moved = pltpu.roll(ref[:, pl.ds(at, BLK)], lax.rem(BLK + 8 * s - inner, BLK), 1)
            rows = jnp.where(lane // 8 == s, moved, rows)
        return rows

    acc_ref[...] = cdot(rows_of(near_ref), near_ref[...]) + cdot(rows_of(far_ref), far_ref[...])
    for s in range(B):
        for m in range(B):
            col = pl.multiple_of(lax.rem(s + m, B) * width + c * BLK, BLK)
            piece = acc_ref[8 * s : 8 * s + 8, pl.ds(col, BLK)]
            base = gram_ref[:, m * BLK : (m + 1) * BLK] if s == 0 else 0.0
            out_ref[s, :, m * BLK : (m + 1) * BLK] = base - piece


def squares(ids, near, far, gram):
    cols = near.shape[1]
    return pl.pallas_call(
        squares_body,
        out_shape=jax.ShapeDtypeStruct((B, 8, cols // 2), F32),
        in_specs=[SMEM, VMEM, VMEM, VMEM],
        out_specs=VMEM,
        scratch_shapes=[pltpu.VMEM((BLK, cols), F32)],
        compiler_params=params(24),
        name="squares",
    )(ids, near, far, gram)


def project_body(ids_ref, near_ref, far_ref, basis_ref, panel_ref, out_ref):
    left = jnp.concatenate([near_ref[...], far_ref[...]], 0)
    right = basis_ref[...]
    (h, m), (p, q) = two(left), two(right)
    left, right = jnp.concatenate([h, h, m], 0), jnp.concatenate([p, q, p], 0)
    out_ref[...] = lax.dot_general(left, right, (((0,), (0,)), ((), ())), preferred_element_type=F32)

    @pl.when(pl.program_id(0) == 0)
    def _():
        out_ref[...] = out_ref[...] - panel_ref[...]


def project(ids, near, far, stacked, panel):
    half, cols = near.shape
    rows, pts = panel.shape
    return pl.pallas_call(
        project_body,
        out_shape=jax.ShapeDtypeStruct((cols, pts), F32),
        grid_spec=pltpu.PrefetchScalarGridSpec(
            num_scalar_prefetch=1,
            grid=(B,),
            in_specs=[
                pl.BlockSpec((half, rows), lambda s, ids: (0, s)),
                pl.BlockSpec((half, rows), lambda s, ids: (0, s)),
                pl.BlockSpec((2 * half, pts), lambda s, ids: (0, 0)),
                pl.BlockSpec((rows, pts), lambda s, ids: (0, 0)),
            ],
            out_specs=pl.BlockSpec((rows, pts), lambda s, ids: (lax.rem(ids[0] + s, B), 0)),
        ),
        compiler_params=params(32),
        name="project",
    )(ids, near, far, stacked, panel)


def lane_splat(tile, c):
    lane = lax.broadcasted_iota(jnp.int32, tile.shape, 1)
    return jnp.broadcast_to(jnp.sum(jnp.where(lane == c, tile, 0.0), axis=1, keepdims=True), tile.shape)


def row_splat(tile, k):
    return jnp.broadcast_to(tile[k : k + 1, :], tile.shape)


def unit_inverse(tiles):
    n = len(tiles)
    tiles = list(tiles)
    sub = lax.broadcasted_iota(jnp.int32, (8, BLK), 0)
    lane = lax.broadcasted_iota(jnp.int32, (8, BLK), 1)
    zero = jnp.zeros((8, BLK), F32)
    one = jnp.ones((8, BLK), F32)
    scale = [None] * n
    for jb in range(n):
        j0 = 8 * jb
        inside = (lane >= j0) & (lane < j0 + 8)
        cols = {r: [lane_splat(tiles[r], j0 + k) for k in range(8)] for r in range(jb, n)}
        panel = jnp.where(inside, jnp.where(lane - j0 == sub, one, zero), tiles[jb])
        mult = {r: [None] * 8 for r in range(jb, n)}
        rows = []
        diag = zero
        for k in range(8):
            pivot = row_splat(cols[jb][k], k)
            recip = 1.0 / pivot
            diag = jnp.where(sub == k, pivot, diag)
            row = row_splat(panel, k)
            rows.append(row)
            for r in range(jb, n):
                m = cols[r][k] * recip
                mult[r][k] = jnp.where(sub > k, m, zero) if r == jb else m
            if k < 7:
                panel = panel - mult[jb][k] * row
            for q in range(k + 1, 8):
                f = row_splat(cols[jb][q], k)
                for r in range(jb, n):
                    cols[r][q] = cols[r][q] - mult[r][k] * f
        for r in range(jb + 1, n):
            a = jnp.where(inside, zero, tiles[r])
            for k in range(8):
                a = a - mult[r][k] * rows[k]
            tiles[r] = a
        tiles[jb] = panel
        scale[jb] = lax.rsqrt(diag)
    return [jnp.where(lane <= 8 * r + sub, tiles[r], zero) * scale[r] for r in range(n)]


def three(x):
    high = x.astype(jnp.bfloat16)
    rest = x - high.astype(F32)
    mid = rest.astype(jnp.bfloat16)
    return high, mid, (rest - mid.astype(F32)).astype(jnp.bfloat16)


def six(left, right, axis):
    (h, m, l), (p, q, r) = left, right
    return jnp.concatenate([h, h, m, h, l, m], axis), jnp.concatenate([p, q, p, r, p, q], 0)


def factor_body(ids_ref, near_ref, far_ref, out_ref, m_ref, s_ref):
    b, c, x, z = ids_ref[0], ids_ref[1], ids_ref[2], ids_ref[3]
    nb = m_ref.shape[0]
    per_band = nb // B
    wide = 2
    for dc, ref in ((0, near_ref), (1, far_ref)):
        cc = lax.rem(c + dc, C)

        def take(t, carry):
            xx = lax.rem(x + t // Z, X)
            zz = z_at(z, lax.rem(t, Z))
            for db in range(B):
                bb = lax.rem(b + db, B)
                row = pl.multiple_of(bb * (per_band * BLK) + (xx * Z + zz) * 8, 8)
                for m in range(nb // 2):
                    col = lax.rem(bb + m, B) * per_band + cc
                    m_ref[col, pl.ds(row, 8), :] = ref[t * B + db, :, m * BLK : (m + 1) * BLK]
            return carry

        lax.fori_loop(0, X * Z, take, 0)

    def step(k, carry):
        base = pl.multiple_of(k * BLK, BLK)
        tiles = [m_ref[k, pl.ds(base + 8 * r, 8), :] for r in range(BLK // 8)]
        inv = jnp.concatenate(unit_inverse(tiles), 0)
        line = jnp.concatenate([m_ref[cb, pl.ds(base, BLK), :] for cb in range(nb)], 1)
        left, right = six(three(inv), three(line), 1)
        prod = jnp.dot(left, right, preferred_element_type=F32)
        blocks = [jnp.where(cb == k, inv, prod[:, cb * BLK : (cb + 1) * BLK]) for cb in range(nb)]

        @pl.when(k // per_band == b)
        def _():
            at = pl.multiple_of(lax.rem(k, per_band) * BLK, BLK)
            for cb in range(nb):
                out_ref[pl.ds(at, BLK), cb * BLK : (cb + 1) * BLK] = jnp.where(cb <= k, -blocks[cb], 0.0)

        for cb in range(nb):
            for i, term in enumerate(three(blocks[cb])):
                s_ref[cb, i * BLK : (i + 1) * BLK] = term
        m_ref[k] = jnp.zeros(m_ref.shape[1:], F32)

        def terms(x):
            return x[:BLK], x[BLK : 2 * BLK], x[2 * BLK :]

        def trail(i, carry):
            ib = pl.multiple_of(i * wide * BLK, wide * BLK)
            full = jnp.concatenate([s_ref[cb] for cb in range(nb)], 1)
            some = jnp.concatenate([s_ref[i * wide + w] for w in range(wide)], 1)
            left, right = six(terms(some), terms(full), 0)
            update = lax.dot_general(left, right, (((0,), (0,)), ((), ())), preferred_element_type=F32)
            for cb in range(nb):
                m_ref[cb, pl.ds(ib, wide * BLK), :] = (
                    m_ref[cb, pl.ds(ib, wide * BLK), :] - update[:, cb * BLK : (cb + 1) * BLK]
                )
            return carry

        lax.fori_loop((k + 1) // wide, jnp.where(k == nb - 1, 0, nb // wide), trail, 0)
        return carry

    lax.fori_loop(0, nb, step, 0)


def factor_rows(ids, near, far, n):
    return pl.pallas_call(
        factor_body,
        out_shape=jax.ShapeDtypeStruct((n // B, n), F32),
        in_specs=[SMEM, VMEM, VMEM],
        out_specs=VMEM,
        scratch_shapes=[pltpu.VMEM((n // BLK, n, BLK), F32), pltpu.VMEM((n // BLK, 3 * BLK, BLK), jnp.bfloat16)],
        compiler_params=params(40),
        name="factor_rows",
    )(ids, near, far)


def ring4(piece, axis):
    half = piece.shape[0] // 2
    after = shift(piece, axis, 4, -1)
    before = shift(piece, axis, 4, 1)
    low = shift(after[:half], axis, 4, -1)
    high = shift(before[half:], axis, 4, 1)
    return [piece, after, jnp.concatenate([low, high], 0), before]


def gather_z(piece):
    pair = jnp.concatenate([piece, shift(piece, "z", Z, 4)], 0)
    return jnp.concatenate([pair] + [shift(pair, "z", Z, by) for by in (-1, -2, 1)], 0)


def reduce_z(rows):
    pairs = rows.reshape(4, -1, rows.shape[1])
    total = pairs[0]
    for e, by in ((1, 1), (2, 2), (3, -1)):
        total = total + shift(pairs[e], "z", Z, by)
    half = total.shape[0] // 2
    return total[:half] + shift(total[half:], "z", Z, 4)


def reduce_core_x(parts, rows_q, first):
    half = rows_q // 2
    low = [part[rows_q:, :BLK] for part in parts]
    high = [part[rows_q:, BLK:] for part in parts]
    keep = [part[:half] for part in parts] + [jnp.where(first, a, d) for a, d in zip(low, high)]
    give = [part[half:rows_q] for part in parts] + [jnp.where(first, d, a) for a, d in zip(low, high)]
    mine = jnp.concatenate(keep, 1) + shift(jnp.concatenate(give, 1), "c", C, 1)
    mine = mine.reshape(X, -1, mine.shape[1])
    mid = mine.shape[1] // 2
    across = jnp.concatenate([shift(mine[2, :mid], "x", X, 2), shift(mine[2, mid:], "x", X, -2)], 0)
    return mine[0] + shift(mine[1], "x", X, 1) + shift(mine[3], "x", X, -1) + across


def body(basis, panel):
    rows_p, pts = panel.shape
    rows_q = basis.shape[0]
    n_panel = rows_p * B
    n_grid = pts * Z * X * C
    first = lax.axis_index("c") == 0
    ids = jnp.stack([lax.axis_index(a) for a in ("b", "c", "x", "z")]).astype(jnp.int32)
    chunks = ring4(panel, "b")
    stacked = rotate(ids, basis, panel)
    groups = ((0,), (1, 3), (2,))
    reduced = []
    for group in groups:
        parts = [tdot(stacked, chunks[s]) for s in group]
        reduced.append(reduce_core_x(parts, rows_q, first))
    total = reduce_z(jnp.concatenate(reduced, 1)) / n_grid
    coeff_at, gram_at, at = ({}, {}, 0)
    for group in groups:
        for s in group:
            coeff_at[s], at = (at, at + rows_p)
        for s in group:
            gram_at[s], at = (at, at + BLK)
    own = jnp.concatenate([total[:, coeff_at[s] : coeff_at[s] + rows_p] for s in range(B)], 1)
    own_gram = jnp.concatenate([total[:, gram_at[s] : gram_at[s] + BLK] for s in range(B)], 1)

    own = gather_z(own)
    near = jnp.concatenate(ring4(own, "x"), 0)
    far = shift(near, "c", C, 1)

    piece = squares(ids, near, far, own_gram)
    gram = piece
    for d in range(1, B):
        gram = gram + jnp.roll(shift(piece, "b", B, -d), d, 0)
    gram, short = lax.optimization_barrier((gram, project(ids, near, far, stacked, panel)))
    short = lax.psum(short, "b")
    gram = gather_z(gram.reshape(B * 8, -1))
    near_gram = jnp.concatenate(ring4(gram, "x"), 0)
    far_gram = shift(near_gram, "c", C, 1)

    coeffs = unrotate(ids, near, far)
    tiled = (-1, 8, near_gram.shape[1])
    rows = factor_rows(ids, near_gram.reshape(tiled), far_gram.reshape(tiled), n_panel)
    new_panel = jnp.dot(rows, short, precision=lax.Precision.HIGH, preferred_element_type=F32)
    return (new_panel, coeffs)


def solution(mesh):
    fine = Mesh(mesh.devices.reshape(Z, X, C, B), GRID + ("b",))
    placed = (P("b", GRID), P("b", GRID))
    return jax.shard_map(
        body,
        mesh=fine,
        in_specs=placed,
        out_specs=(P("b", GRID), P("b", None)),
        check_vma=False,
    )
```
